32 devices in a mesh: groups: 2 (over y), row: 4 (over z), col: 2 (over x), sub: 2 (over core).
Axes of the slice: x: 2, y: 2, z: 4, core: 2. Of those that a mesh axis runs over, the one named last changes fastest.
Arguments:
- matrix: float32 [16384, 8192], P(('groups', 'row'), ('col', 'sub')), parts along dimension 0, may hold values from -60 to 60
- basis_vectors: float32 [16384, 1024], P(('groups', 'row'), ('col', 'sub')), parts along dimension 0, may hold values from -0.0625 to 0.0625
- split_size: int32 [2], P('groups'), parts along dimension 0, may hold values from 256 to 767
Outputs:
- children: float32 [2, 2048, 1024], P('sub', ('groups', 'row'), 'col'), parts along dimension 1
The draws below stay inside these ranges and needn't reach their ends.
There are 2 independent parts, one for each index of `groups`. The reference program is written for one: setup_inputs(seed, part) draws one part's arguments, and reference() takes and returns one part's arrays. A program takes and returns all parts, laid end to end along the dimension named above; each array names one. Nothing has to cross between parts.
Inputs may be any that keep to these rules, and one draw needn't show every extreme that they name: The second subspace has 1024 minus split_size vectors.
All inputs are finite; a program needn't handle non-finite values.
Results may differ from the reference program's by a relative error of at most 0.00011.
Values sent between devices are 32-bit elements; how exact they have to be, the bound alone decides.
A program may use at most 128 MiB of HBM per device.

```python
import jax
import jax.numpy as jnp
from jax import lax

N = 8192
K = 1024


def draw_matrix(key, part):
    noise = jax.random.normal(key, (N, N), jnp.float32)
    symmetric = (noise + noise.T) * 0.5 ** 0.5
    return symmetric


def level_of(stream_key, dims, split, least, top_value):
    loudness = 1.0
    for position, parts in split:
        steps = jax.random.uniform(jax.random.fold_in(jax.random.fold_in(stream_key, 6), position), (parts,), jnp.float32, least / len(split), top_value / len(split))
        loudness = loudness * jnp.repeat(jnp.exp(steps), dims[position] // parts).reshape((-1,) + (1,) * (len(dims) - 1 - position))
    return loudness


def gaussian(own_key, shape, spread, most, pieces=(), kind=jnp.bfloat16):
    result = jax.random.normal(own_key, shape, jnp.float32) * spread
    if len(pieces) > 0:
        result = level_of(own_key, shape, pieces, -0.22, 0.18) * result
    return jnp.clip(result, min=-most, max=most).astype(kind)


def setup_inputs(seed: int = 0, part: int = 0) -> dict:
    splits = jax.random.split(jax.random.key(seed), 4)
    part_keys = jax.random.split(jax.random.fold_in(splits[3], part), 4)
    return {
        "matrix": draw_matrix(jax.random.fold_in(jax.random.fold_in(splits[3], part), 71), part),
        "basis_vectors": gaussian(part_keys[1], (N, K), N ** -0.5, 0.0625, ((0, 4), (1, 4)), jnp.float32),
        "split_size": jax.random.randint(part_keys[2], (1,), K // 4, 3 * K // 4).astype(jnp.int32),
    }


def reference(matrix, basis_vectors, split_size):
    image = jnp.dot(matrix, basis_vectors, precision=lax.Precision.HIGHEST, preferred_element_type=jnp.float32)
    projected = jnp.dot(basis_vectors.T, image, precision=lax.Precision.HIGHEST, preferred_element_type=jnp.float32)
    positions = jnp.arange(K, dtype=jnp.int32)
    in_first = positions < split_size[0]
    in_second = jnp.logical_not(in_first)
    mask_one = in_first[:, None] & in_first[None, :]
    mask_two = in_second[:, None] & in_second[None, :]
    nothing = jnp.zeros((), jnp.float32)
    return jnp.stack([jnp.where(mask_one, projected, nothing), jnp.where(mask_two, projected, nothing)])
```

```python
import jax
import jax.numpy as jnp
from jax import lax
from jax.sharding import PartitionSpec as P


def shards(matrix, basis_vectors, split_size):
    R = lax.axis_size("row")
    S = lax.axis_size("sub")
    C = lax.axis_size("col") * S
    m, kd = basis_vectors.shape
    K = kd * C
    n = matrix.shape[1]
    per = n // m
    piece = m // R
    spread = lax.all_to_all(basis_vectors, "row", split_axis=0, concat_axis=0, tiled=True)
    mine = lax.all_to_all(spread, ("col", "sub"), split_axis=0, concat_axis=1, tiled=True)
    own = lax.all_gather(basis_vectors, ("col", "sub"), axis=1, tiled=True)
    part = lax.dot_general(
        matrix,
        own,
        (((0,), (0,)), ((), ())),
        precision=lax.Precision.HIGH,
        preferred_element_type=jnp.float32,
    )
    part = part.reshape(per, R, piece, K).transpose(1, 0, 2, 3).reshape(R * per * piece, K)
    image = lax.psum_scatter(part, "row", scatter_dimension=0, tiled=True)
    partial_proj = lax.dot_general(
        mine,
        image,
        (((0,), (0,)), ((), ())),
        precision=lax.Precision.HIGH,
        preferred_element_type=jnp.float32,
    )
    proj = lax.psum_scatter(partial_proj, "row", scatter_dimension=0, tiled=True)
    proj = lax.psum_scatter(proj, ("col", "sub"), scatter_dimension=1, tiled=True)
    child_block = lax.all_gather(proj, "sub", axis=1, tiled=True)
    row_ids = (
        jnp.arange(child_block.shape[0], dtype=jnp.int32)
        + lax.axis_index("row") * child_block.shape[0]
    )
    col_ids = (
        jnp.arange(child_block.shape[1], dtype=jnp.int32)
        + lax.axis_index("col") * child_block.shape[1]
    )
    leading = split_size[0]
    row_first = row_ids < leading
    col_first = col_ids < leading
    mask_one = row_first[:, None] & col_first[None, :]
    mask_two = jnp.logical_not(row_first)[:, None] & jnp.logical_not(col_first)[None, :]
    selected = jnp.where(lax.axis_index("sub") == 0, mask_one, mask_two)
    return jnp.where(selected, child_block, jnp.zeros((), jnp.float32))[None]


def solution(mesh):
    placed = (
        P(("groups", "row"), ("col", "sub")),
        P(("groups", "row"), ("col", "sub")),
        P("groups"),
    )
    return jax.shard_map(
        shards,
        mesh=mesh,
        in_specs=placed,
        out_specs=P("sub", ("groups", "row"), "col"),
        check_vma=False,
    )
```

```python
import functools

import jax
import jax.numpy as jnp
from jax import lax
from jax.experimental import pallas as pl
from jax.experimental.pallas import tpu as pltpu
from jax.sharding import PartitionSpec as P

MESH = pl.DeviceIdType.MESH
CHUNKS = 2


def gather_kernel(R, X, S, v, own, spread, lsem, xs, xr, zs, zr, ps, pr, fs, fr):
    r, x, s = lax.axis_index("row"), lax.axis_index("col"), lax.axis_index("sub")
    m, kd = v.shape
    piece = m // R

    def columns(cx, cs):
        return pl.ds(pl.multiple_of((cx * S + cs) * kd, kd), kd)

    peers = [{"col": lax.rem(x + d, X)} for d in range(1, X)]
    peers += [{"row": lax.rem(r + d, R)} for d in range(1, R)]
    peers += [{"sub": lax.rem(s + d, S)} for d in range(1, S)]
    barrier = pltpu.get_barrier_semaphore()
    for peer in peers:
        pl.semaphore_signal(barrier, inc=1, device_id=peer, device_id_type=MESH)
    pl.semaphore_wait(barrier, len(peers))

    mine = own.at[:, columns(x, s)]
    across, spreads, partner, forward = [], [], [], []
    for d in range(1, X):
        across.append(pltpu.make_async_remote_copy(
            v, mine, xs.at[d - 1], xr.at[d - 1],
            device_id={"col": lax.rem(x + d, X)}, device_id_type=MESH))
    for d in range(1, R):
        i = lax.rem(r + d, R)
        spreads.append(pltpu.make_async_remote_copy(
            v.at[pl.ds(pl.multiple_of(i * piece, piece), piece), :], spread.at[r],
            zs.at[d - 1], zr.at[d - 1],
            device_id={"row": i}, device_id_type=MESH))
    for d in range(1, S):
        partner.append(pltpu.make_async_remote_copy(
            v, mine, ps.at[d - 1], pr.at[d - 1],
            device_id={"sub": lax.rem(s + d, S)}, device_id_type=MESH))
    for copy in across + spreads + partner:
        copy.start()
    local = [
        pltpu.make_async_copy(v, mine, lsem.at[0]),
        pltpu.make_async_copy(
            v.at[pl.ds(pl.multiple_of(r * piece, piece), piece), :], spread.at[r], lsem.at[1]),
    ]
    for copy in local:
        copy.start()
    for d in range(1, X):
        across[d - 1].wait_recv()
        block = own.at[:, columns(lax.rem(x - d + X, X), s)]
        for e in range(1, S):
            copy = pltpu.make_async_remote_copy(
                block, block, fs.at[d - 1, e - 1], fr.at[d - 1, e - 1],
                device_id={"sub": lax.rem(s + e, S)}, device_id_type=MESH)
            copy.start()
            forward.append(copy)
    for copy in across:
        copy.wait_send()
    for copy in spreads + partner + forward:
        copy.wait()
    for copy in local:
        copy.wait()


def gather(v, R, X, S):
    m, kd = v.shape
    dma = pltpu.SemaphoreType.DMA
    return pl.pallas_call(
        functools.partial(gather_kernel, R, X, S),
        out_shape=(
            jax.ShapeDtypeStruct((m, kd * X * S), v.dtype),
            jax.ShapeDtypeStruct((R, m // R, kd), v.dtype),
        ),
        in_specs=[pl.BlockSpec(memory_space=pltpu.VMEM)],
        out_specs=(pl.BlockSpec(memory_space=pl.ANY), pl.BlockSpec(memory_space=pl.ANY)),
        scratch_shapes=[
            dma((2,)), dma((X - 1,)), dma((X - 1,)), dma((R - 1,)), dma((R - 1,)),
            dma((S - 1,)), dma((S - 1,)), dma((X - 1, S - 1)), dma((X - 1, S - 1)),
        ],
        compiler_params=pltpu.CompilerParams(collective_id=0, has_side_effects=True),
        cost_estimate=pl.CostEstimate(flops=0, bytes_accessed=100_000_000, transcendentals=0),
        name="gather",
    )(v)


def regroup_kernel(X, S, spread, mine, lsem, ss, rs):
    x, s = lax.axis_index("col"), lax.axis_index("sub")
    C = X * S
    k = x * S + s
    R, piece, kd = spread.shape
    per = R // C
    barrier = pltpu.get_barrier_semaphore()
    dests = [lax.rem(k + e, C) for e in range(C)]
    for j in dests[1:]:
        pl.semaphore_signal(
            barrier, inc=1, device_id={"col": j // S, "sub": lax.rem(j, S)}, device_id_type=MESH)
    pl.semaphore_wait(barrier, C - 1)
    target = mine.at[:, :, pl.ds(pl.multiple_of(k * kd, kd), kd)]
    copies = []
    for e in range(1, C):
        j = dests[e]
        copies.append(pltpu.make_async_remote_copy(
            spread.at[pl.ds(j * per, per)], target, ss.at[e - 1], rs.at[e - 1],
            device_id={"col": j // S, "sub": lax.rem(j, S)}, device_id_type=MESH))
    copies.append(pltpu.make_async_copy(spread.at[pl.ds(k * per, per)], target, lsem))
    for copy in copies:
        copy.start()
    for copy in copies:
        copy.wait()


def regroup(spread, X, S):
    R, piece, kd = spread.shape
    C = X * S
    dma = pltpu.SemaphoreType.DMA
    return pl.pallas_call(
        functools.partial(regroup_kernel, X, S),
        out_shape=jax.ShapeDtypeStruct((R // C, piece, kd * C), spread.dtype),
        in_specs=[pl.BlockSpec(memory_space=pltpu.VMEM)],
        out_specs=pl.BlockSpec(memory_space=pl.ANY),
        scratch_shapes=[dma, dma((C - 1,)), dma((C - 1,))],
        compiler_params=pltpu.CompilerParams(collective_id=1, has_side_effects=True),
        cost_estimate=pl.CostEstimate(flops=0, bytes_accessed=60_000_000, transcendentals=0),
        name="regroup",
    )(spread)


def shards(matrix, basis_vectors, split_size):
    R = lax.axis_size("row")
    S = lax.axis_size("sub")
    C = lax.axis_size("col") * S
    m, kd = basis_vectors.shape
    K = kd * C
    n = matrix.shape[1]
    per = n // m
    piece = m // R
    own, spread = gather(basis_vectors, R, C // S, S)
    width = K // CHUNKS
    images = []
    for c in range(CHUNKS):
        part = lax.dot_general(
            matrix,
            own[:, c * width : (c + 1) * width],
            (((0,), (0,)), ((), ())),
            precision=lax.Precision.HIGH,
            preferred_element_type=jnp.float32,
        )
        if c == 0:
            part, spread = lax.optimization_barrier((part, spread))
        part = part.reshape(per, R, piece, width).transpose(1, 0, 2, 3).reshape(R * per * piece, width)
        images.append(lax.psum_scatter(part, "row", scatter_dimension=0, tiled=True))
    mine = regroup(spread, C // S, S).reshape(per * piece, K)
    partial_proj = jnp.concatenate(
        [
            lax.dot_general(
                mine,
                image,
                (((0,), (0,)), ((), ())),
                precision=lax.Precision.HIGH,
                preferred_element_type=jnp.float32,
            )
            for image in images
        ],
        axis=1,
    )
    proj = lax.psum_scatter(partial_proj, "row", scatter_dimension=0, tiled=True)
    proj = lax.psum_scatter(proj, ("col", "sub"), scatter_dimension=1, tiled=True)
    child_block = lax.all_gather(proj, "sub", axis=1, tiled=True)
    row_ids = (
        jnp.arange(child_block.shape[0], dtype=jnp.int32)
        + lax.axis_index("row") * child_block.shape[0]
    )
    col_ids = (
        jnp.arange(child_block.shape[1], dtype=jnp.int32)
        + lax.axis_index("col") * child_block.shape[1]
    )
    leading = split_size[0]
    row_first = row_ids < leading
    col_first = col_ids < leading
    mask_one = row_first[:, None] & col_first[None, :]
    mask_two = jnp.logical_not(row_first)[:, None] & jnp.logical_not(col_first)[None, :]
    selected = jnp.where(lax.axis_index("sub") == 0, mask_one, mask_two)
    return jnp.where(selected, child_block, jnp.zeros((), jnp.float32))[None]


def solution(mesh):
    placed = (
        P(("groups", "row"), ("col", "sub")),
        P(("groups", "row"), ("col", "sub")),
        P("groups"),
    )
    return jax.shard_map(
        shards,
        mesh=mesh,
        in_specs=placed,
        out_specs=P("sub", ("groups", "row"), "col"),
        check_vma=False,
    )
```

```python
import functools

import jax
import jax.numpy as jnp
from jax import lax
from jax.experimental import pallas as pl
from jax.experimental.pallas import tpu as pltpu
from jax.sharding import PartitionSpec as P

MESH = pl.DeviceIdType.MESH
CHUNKS = 1


def gather_kernel(R, X, S, v, own, spread, lsem, xs, xr, zs, zr, ps, pr, fs, fr):
    r, x, s = lax.axis_index("row"), lax.axis_index("col"), lax.axis_index("sub")
    m, kd = v.shape
    piece = m // R

    def columns(cx, cs):
        return pl.ds(pl.multiple_of((cx * S + cs) * kd, kd), kd)

    peers = [{"col": lax.rem(x + d, X)} for d in range(1, X)]
    peers += [{"row": lax.rem(r + d, R)} for d in range(1, R)]
    peers += [{"sub": lax.rem(s + d, S)} for d in range(1, S)]
    barrier = pltpu.get_barrier_semaphore()
    for peer in peers:
        pl.semaphore_signal(barrier, inc=1, device_id=peer, device_id_type=MESH)
    pl.semaphore_wait(barrier, len(peers))

    mine = own.at[:, columns(x, s)]
    across, spreads, partner, forward = [], [], [], []
    for d in range(1, X):
        across.append(pltpu.make_async_remote_copy(
            v, mine, xs.at[d - 1], xr.at[d - 1],
            device_id={"col": lax.rem(x + d, X)}, device_id_type=MESH))
    for d in range(1, R):
        i = lax.rem(r + d, R)
        spreads.append(pltpu.make_async_remote_copy(
            v.at[pl.ds(pl.multiple_of(i * piece, piece), piece), :], spread.at[r],
            zs.at[d - 1], zr.at[d - 1],
            device_id={"row": i}, device_id_type=MESH))
    for d in range(1, S):
        partner.append(pltpu.make_async_remote_copy(
            v, mine, ps.at[d - 1], pr.at[d - 1],
            device_id={"sub": lax.rem(s + d, S)}, device_id_type=MESH))
    for copy in across + spreads + partner:
        copy.start()
    local = [
        pltpu.make_async_copy(v, mine, lsem.at[0]),
        pltpu.make_async_copy(
            v.at[pl.ds(pl.multiple_of(r * piece, piece), piece), :], spread.at[r], lsem.at[1]),
    ]
    for copy in local:
        copy.start()
    for d in range(1, X):
        across[d - 1].wait_recv()
        block = own.at[:, columns(lax.rem(x - d + X, X), s)]
        for e in range(1, S):
            copy = pltpu.make_async_remote_copy(
                block, block, fs.at[d - 1, e - 1], fr.at[d - 1, e - 1],
                device_id={"sub": lax.rem(s + e, S)}, device_id_type=MESH)
            copy.start()
            forward.append(copy)
    for copy in across:
        copy.wait_send()
    for copy in spreads + partner + forward:
        copy.wait()
    for copy in local:
        copy.wait()


def gather(v, R, X, S):
    m, kd = v.shape
    dma = pltpu.SemaphoreType.DMA
    return pl.pallas_call(
        functools.partial(gather_kernel, R, X, S),
        out_shape=(
            jax.ShapeDtypeStruct((m, kd * X * S), v.dtype),
            jax.ShapeDtypeStruct((R, m // R, kd), v.dtype),
        ),
        in_specs=[pl.BlockSpec(memory_space=pltpu.VMEM)],
        out_specs=(pl.BlockSpec(memory_space=pl.ANY), pl.BlockSpec(memory_space=pl.ANY)),
        scratch_shapes=[
            dma((2,)), dma((X - 1,)), dma((X - 1,)), dma((R - 1,)), dma((R - 1,)),
            dma((S - 1,)), dma((S - 1,)), dma((X - 1, S - 1)), dma((X - 1, S - 1)),
        ],
        compiler_params=pltpu.CompilerParams(collective_id=0, has_side_effects=True),
        cost_estimate=pl.CostEstimate(flops=0, bytes_accessed=100_000_000, transcendentals=0),
        name="gather",
    )(v)


def regroup_kernel(X, S, spread, mine, lsem, ss, rs):
    x, s = lax.axis_index("col"), lax.axis_index("sub")
    C = X * S
    k = x * S + s
    R, piece, kd = spread.shape
    per = R // C
    barrier = pltpu.get_barrier_semaphore()
    dests = [lax.rem(k + e, C) for e in range(C)]
    for j in dests[1:]:
        pl.semaphore_signal(
            barrier, inc=1, device_id={"col": j // S, "sub": lax.rem(j, S)}, device_id_type=MESH)
    pl.semaphore_wait(barrier, C - 1)
    target = mine.at[:, :, pl.ds(pl.multiple_of(k * kd, kd), kd)]
    copies = []
    for e in range(1, C):
        j = dests[e]
        copies.append(pltpu.make_async_remote_copy(
            spread.at[pl.ds(j * per, per)], target, ss.at[e - 1], rs.at[e - 1],
            device_id={"col": j // S, "sub": lax.rem(j, S)}, device_id_type=MESH))
    copies.append(pltpu.make_async_copy(spread.at[pl.ds(k * per, per)], target, lsem))
    for copy in copies:
        copy.start()
    for copy in copies:
        copy.wait()


def regroup(spread, X, S):
    R, piece, kd = spread.shape
    C = X * S
    dma = pltpu.SemaphoreType.DMA
    return pl.pallas_call(
        functools.partial(regroup_kernel, X, S),
        out_shape=jax.ShapeDtypeStruct((R // C, piece, kd * C), spread.dtype),
        in_specs=[pl.BlockSpec(memory_space=pltpu.VMEM)],
        out_specs=pl.BlockSpec(memory_space=pl.ANY),
        scratch_shapes=[dma, dma((C - 1,)), dma((C - 1,))],
        compiler_params=pltpu.CompilerParams(collective_id=1, has_side_effects=True),
        cost_estimate=pl.CostEstimate(flops=0, bytes_accessed=60_000_000, transcendentals=0),
        name="regroup",
    )(spread)


def project_kernel(R, X, S, p, out, acc, from_sub, from_col, from_row, res, from_pair,
                   a_s, a_r, b_s, b_r, c_s, c_r, d_s, d_r):
    r, x, s = lax.axis_index("row"), lax.axis_index("col"), lax.axis_index("sub")
    K = p.shape[0]
    rb, kd = K // R, K // (X * S)

    def rows(i):
        return pl.ds(pl.multiple_of(i * rb, rb), rb)

    def columns(cx, cs):
        return pl.ds(pl.multiple_of((cx * S + cs) * kd, kd), kd)

    def col(d):
        return lax.rem(x + d, X)

    peers = [{"col": col(d)} for d in range(1, X)]
    peers += [{"row": lax.rem(r + d, R)} for d in range(1, R)]
    peers += [{"sub": lax.rem(s + d, S)} for d in range(1, S)]
    barrier = pltpu.get_barrier_semaphore()
    for peer in peers:
        pl.semaphore_signal(barrier, inc=1, device_id=peer, device_id_type=MESH)
    pl.semaphore_wait(barrier, len(peers))

    order = list(range(1, X)) + [0]
    steps = list(range(1, R)) + [0]
    pair = {}
    for d in order:
        for e in range(1, S):
            other = lax.rem(s + e, S)
            pair[d, e] = pltpu.make_async_remote_copy(
                p.at[:, columns(col(d), other)], from_sub.at[e - 1, d],
                a_s.at[e - 1, d], a_r.at[e - 1, d],
                device_id={"sub": other}, device_id_type=MESH)
            pair[d, e].start()
    cross = {}
    for d in order:
        for e in range(1, S):
            pair[d, e].wait_recv()
        for q in steps:
            here = rows(lax.rem(r + q, R))
            total = p[here, columns(col(d), s)]
            for e in range(1, S):
                total = total + from_sub[e - 1, d, here, :]
            acc[d, here, :] = total
            if d > 0:
                cross[d, q] = pltpu.make_async_remote_copy(
                    acc.at[d, here], from_col.at[d - 1, here],
                    b_s.at[d - 1, q], b_r.at[d - 1, q],
                    device_id={"col": col(d)}, device_id_type=MESH)
                cross[d, q].start()
    along = []
    for q in steps:
        i = lax.rem(r + q, R)
        here = rows(i)
        total = acc[0, here, :]
        for d in range(1, X):
            cross[d, q].wait_recv()
            total = total + from_col[d - 1, here, :]
        if q > 0:
            acc[0, here, :] = total
            copy = pltpu.make_async_remote_copy(
                acc.at[0, here], from_row.at[q - 1], c_s.at[q - 1], c_r.at[q - 1],
                device_id={"row": i}, device_id_type=MESH)
            copy.start()
            along.append(copy)
    for q in range(1, R):
        along[q - 1].wait_recv()
        total = total + from_row[q - 1]
    res[...] = total
    last = []
    for e in range(1, S):
        copy = pltpu.make_async_remote_copy(
            res, from_pair.at[e - 1], d_s.at[e - 1], d_r.at[e - 1],
            device_id={"sub": lax.rem(s + e, S)}, device_id_type=MESH)
        copy.start()
        last.append(copy)
    out[:, pl.ds(pl.multiple_of(s * kd, kd), kd)] = total
    for e in range(1, S):
        last[e - 1].wait_recv()
        out[:, pl.ds(pl.multiple_of(lax.rem(s - e + S, S) * kd, kd), kd)] = from_pair[e - 1]
    for copy in list(pair.values()) + list(cross.values()) + along + last:
        copy.wait_send()


def project(partial, R, X, S):
    K = partial.shape[0]
    rb, kd = K // R, K // (X * S)
    dma = pltpu.SemaphoreType.DMA
    f32 = jnp.float32
    return pl.pallas_call(
        functools.partial(project_kernel, R, X, S),
        out_shape=jax.ShapeDtypeStruct((rb, S * kd), f32),
        in_specs=[pl.BlockSpec(memory_space=pltpu.VMEM)],
        out_specs=pl.BlockSpec(memory_space=pltpu.VMEM),
        scratch_shapes=[
            pltpu.VMEM((X, K, kd), f32),
            pltpu.VMEM((S - 1, X, K, kd), f32),
            pltpu.VMEM((X - 1, K, kd), f32),
            pltpu.VMEM((R - 1, rb, kd), f32),
            pltpu.VMEM((rb, kd), f32),
            pltpu.VMEM((S - 1, rb, kd), f32),
            dma((S - 1, X)), dma((S - 1, X)), dma((X - 1, R)), dma((X - 1, R)),
            dma((R - 1,)), dma((R - 1,)), dma((S - 1,)), dma((S - 1,)),
        ],
        compiler_params=pltpu.CompilerParams(collective_id=2, has_side_effects=True),
        cost_estimate=pl.CostEstimate(flops=0, bytes_accessed=60_000_000, transcendentals=0),
        name="project",
    )(partial)


def shards(matrix, basis_vectors, split_size):
    R = lax.axis_size("row")
    S = lax.axis_size("sub")
    C = lax.axis_size("col") * S
    m, kd = basis_vectors.shape
    K = kd * C
    n = matrix.shape[1]
    per = n // m
    piece = m // R
    own, spread = gather(basis_vectors, R, C // S, S)
    width = K // CHUNKS
    images = []
    for c in range(CHUNKS):
        part = lax.dot_general(
            matrix,
            own[:, c * width : (c + 1) * width],
            (((0,), (0,)), ((), ())),
            precision=lax.Precision.HIGH,
            preferred_element_type=jnp.float32,
        )
        if c == 0:
            part, spread = lax.optimization_barrier((part, spread))
        part = part.reshape(per, R, piece, width).transpose(1, 0, 2, 3).reshape(R * per * piece, width)
        images.append(lax.psum_scatter(part, "row", scatter_dimension=0, tiled=True))
    mine = regroup(spread, C // S, S).reshape(per * piece, K)
    partial_proj = jnp.concatenate(
        [
            lax.dot_general(
                mine,
                image,
                (((0,), (0,)), ((), ())),
                precision=lax.Precision.HIGH,
                preferred_element_type=jnp.float32,
            )
            for image in images
        ],
        axis=1,
    )
    child_block = project(partial_proj, R, C // S, S)
    row_ids = (
        jnp.arange(child_block.shape[0], dtype=jnp.int32)
        + lax.axis_index("row") * child_block.shape[0]
    )
    col_ids = (
        jnp.arange(child_block.shape[1], dtype=jnp.int32)
        + lax.axis_index("col") * child_block.shape[1]
    )
    leading = split_size[0]
    row_first = row_ids < leading
    col_first = col_ids < leading
    mask_one = row_first[:, None] & col_first[None, :]
    mask_two = jnp.logical_not(row_first)[:, None] & jnp.logical_not(col_first)[None, :]
    selected = jnp.where(lax.axis_index("sub") == 0, mask_one, mask_two)
    return jnp.where(selected, child_block, jnp.zeros((), jnp.float32))[None]


def solution(mesh):
    placed = (
        P(("groups", "row"), ("col", "sub")),
        P(("groups", "row"), ("col", "sub")),
        P("groups"),
    )
    return jax.shard_map(
        shards,
        mesh=mesh,
        in_specs=placed,
        out_specs=P("sub", ("groups", "row"), "col"),
        check_vma=False,
    )
```
